128 devices in a mesh: ep: 8 (over z_lo, x), fsdp: 16 (over z_hi, y, core).
Axes of the slice: x: 4, y: 4, z: 4 (z_hi: 2, z_lo: 2; z = z_hi * 2 + z_lo), core: 2. Of those that a mesh axis runs over, the one named last changes fastest.
Arguments:
- train_gate: float32 [64, 2048, 1408], P('ep', 'fsdp'), may hold values from -0.1875 to 0.1875
- other_gate: bfloat16 [64, 2048, 1408], P('ep', 'fsdp'), may hold values from -0.0625 to 0.0625
- train_up: float32 [64, 2048, 1408], P('ep', 'fsdp'), may hold values from -0.1875 to 0.1875
- other_up: bfloat16 [64, 2048, 1408], P('ep', 'fsdp'), may hold values from -0.0625 to 0.0625
- router_weight: float32 [2048, 64], P('fsdp', 'ep'), may hold values from -0.125 to 0.125
- router_gain: float32 [2048], P('fsdp'), may hold values from 0.25 to 1.75
Outputs:
- ready_gate: bfloat16 [64, 2048, 1408], P('ep', None, 'fsdp')
- ready_up: bfloat16 [64, 2048, 1408], P('ep', None, 'fsdp')
- scale_gate: float32 [64, 1408], P('ep', 'fsdp')
- scale_up: float32 [64, 1408], P('ep', 'fsdp')
- serve_router: bfloat16 [2048, 64], replicated
The draws below stay inside these ranges and needn't reach their ends.
All inputs are finite; a program needn't handle non-finite values. Where the reference program divides by a largest or mean magnitude, that divisor is 1e-20 or more.
Results may differ from the reference program's by a relative error of at most 0.001.
Values may be sent and summed in bfloat16 or wider, within the bound.
A program may use at most 128 MiB of HBM per device.

```python
import jax
import jax.numpy as jnp

EXPERTS = 64
D_MODEL = 2048
D_EXPERT = 1408


def strengthened(array, stream_key, source, target, blocks, factor):
    owner, partner = [(jnp.arange(array.shape[axis_at]) // (array.shape[axis_at] // blocks)).reshape([-1 if axis == axis_at else 1 for axis in range(array.ndim)]) for axis_at in (source, target)]
    chosen = jax.random.permutation(stream_key, blocks)[partner]
    strong = (owner == chosen) | (owner == (partner + blocks // 2) % blocks)
    return jnp.where(strong, factor * array, array)


def steps_of(rng, shape, split, smallest, high):
    def one(axis_at, shards_of):
        heights = jax.random.uniform(jax.random.fold_in(jax.random.fold_in(rng, 6), axis_at), (shards_of,), jnp.float32, smallest / len(split), high / len(split))
        return jnp.repeat(jnp.exp(heights), shape[axis_at] // shards_of).reshape((-1,) + (1,) * (len(shape) - axis_at - 1))

    factor_of = one(*split[0])
    for cut in split[1:]:
        factor_of = factor_of * one(*cut)
    return factor_of


def normal_values(own_key, extent, spread, limit, cuts=(), held_as=jnp.bfloat16):
    entries = spread * jax.random.normal(own_key, extent, jnp.float32)
    if cuts:
        entries = entries * steps_of(own_key, extent, cuts, -0.22, 0.18)
    return jnp.clip(entries, -limit, limit).astype(held_as)


def bell_draw_with(stream_key, shape, spread, most, split, heavy, dtype=jnp.bfloat16):
    result = spread * jax.random.normal(stream_key, shape, jnp.float32)
    if split:
        result = result * steps_of(stream_key, shape, split, -0.22, 0.18)
    return jnp.clip(strengthened(result, jax.random.fold_in(stream_key, 3), *heavy), -most, most).astype(dtype)


def setup_inputs(seed: int = 0) -> dict:
    splits = jax.random.split(jax.random.key(seed), 7)
    train_gate = bell_draw_with(splits[0], (EXPERTS, D_MODEL, D_EXPERT), D_MODEL ** -0.5, 0.1875, ((0, 8), (1, 16)), (1, 2, 16, 2.0), jnp.float32)
    other_gate = normal_values(splits[1], (EXPERTS, D_MODEL, D_EXPERT), (D_MODEL * 4) ** -0.5, 0.0625, ((0, 8), (1, 16)))
    train_up = bell_draw_with(splits[2], (EXPERTS, D_MODEL, D_EXPERT), D_MODEL ** -0.5, 0.1875, ((0, 8), (1, 16)), (1, 2, 16, 2.0), jnp.float32)
    other_up = normal_values(splits[3], (EXPERTS, D_MODEL, D_EXPERT), (D_MODEL * 4) ** -0.5, 0.0625, ((0, 8), (1, 16)))
    router_weight = normal_values(splits[4], (D_MODEL, EXPERTS), D_MODEL ** -0.5, 0.125, ((0, 16), (1, 8)), jnp.float32)
    router_gain = jnp.clip(1.0 + 0.15 * jax.random.normal(splits[5], (D_MODEL,), jnp.float32), 0.25, 1.75)
    return dict(train_gate=train_gate, other_gate=other_gate, train_up=train_up, other_up=other_up, router_weight=router_weight, router_gain=router_gain)


def reference(train_gate, other_gate, train_up, other_up, router_weight, router_gain):
    latest_gate = train_gate + other_gate.astype(jnp.float32)
    latest_up = train_up + other_up.astype(jnp.float32)
    scale_gate = jnp.max(jnp.abs(latest_gate), axis=1)
    ready_gate = (latest_gate / jnp.expand_dims(scale_gate, 1)).astype(jnp.bfloat16)
    scale_up = jnp.max(jnp.abs(latest_up), axis=1)
    ready_up = (latest_up / jnp.expand_dims(scale_up, 1)).astype(jnp.bfloat16)
    serve_router = (router_weight * router_gain[:, None]).astype(jnp.bfloat16)
    return ready_gate, ready_up, scale_gate, scale_up, serve_router
```

```python
import functools

import jax
import jax.numpy as jnp
from jax import lax
from jax.experimental import pallas as pl
from jax.experimental.pallas import tpu as pltpu
from jax.sharding import Mesh
from jax.sharding import PartitionSpec as P

MESH = pl.DeviceIdType.MESH
AXES = ("zl", "x", "zh", "y", "c")
EP = ("zl", "x")
FSDP = ("zh", "y", "c")
LANES = 128
PEERS = (
    (1, 1, 0), (3, 1, 0), (0, 1, 0), (2, 1, 0), (1, 0, 0), (3, 0, 0), (2, 0, 0),
    (1, 1, 1), (3, 1, 1), (0, 1, 1), (2, 1, 1), (1, 0, 1), (3, 0, 1), (2, 0, 1), (0, 0, 1),
)


def kernel(
    sizes,
    tg, og, tu, ou, rw, rg,
    gate, up, sg, su, router,
    train, other, turned, blocks, first, firsts, local, parts, scales, tile,
    load_sem, send_sem, recv_sem, own_sem,
    first_send, first_recv, part_send, part_recv, scale_send, scale_recv,
    tile_send, tile_recv, pair_send, pair_recv, row_send, row_recv,
):
    nzl, nx, nzh, ny, nc = sizes
    experts, depth, width = tg.shape
    members = nzh * ny * nc
    cut = width // members
    strips = width // LANES
    zl, x, zh, y, c = (lax.axis_index(a) for a in AXES)
    me = (zh * ny + y) * nc + c
    part = zl * nx + x
    arrays = ((tg, og, gate), (tu, ou, up))

    def load(t, e):
        return (
            pltpu.make_async_copy(arrays[t][0].at[e], train.at[t, e], load_sem.at[0, t, e]),
            pltpu.make_async_copy(arrays[t][1].at[e], other.at[t, e], load_sem.at[1, t, e]),
        )

    def peer(step):
        dy, dz, dc = step
        ty, tz, tc = lax.rem(y + dy, ny), lax.rem(zh + dz, nzh), lax.rem(c + dc, nc)
        return (tz * ny + ty) * nc + tc, (zl, x, tz, ty, tc)

    others = [peer(step) for step in PEERS]
    across = (lax.rem(zl + 1, nzl), x, zh, y, c)
    along = [(zl, lax.rem(x + k, nx), zh, y, c) for k in range(1, nx)]
    mine = pl.ds(pl.multiple_of(me * LANES, LANES), LANES)

    barrier = pltpu.get_barrier_semaphore()
    everyone = [d for _, d in others] + [across] + along
    for d in everyone:
        pl.semaphore_signal(barrier, inc=1, device_id=d, device_id_type=MESH)

    for t in range(2):
        for copy in load(t, 0):
            copy.start()

    @pl.loop(1, experts)
    def _(e):
        for t in range(2):
            for copy in load(t, e):
                copy.start()

    def largest(t, e):
        for copy in load(t, e):
            copy.wait()
        latest = train[t, e] + other[t, e].astype(jnp.float32)
        return jnp.max(jnp.abs(latest), axis=0, keepdims=True)

    for t in range(2):
        top = largest(t, 0)
        for k in range(strips):
            first[t, k : k + 1, :] = top[:, k * LANES : (k + 1) * LANES]
    tile[...] = (rw[...] * rg[...]).astype(tile.dtype)
    firsts[me] = first[...]

    pl.semaphore_wait(barrier, len(everyone))
    for _, d in others:
        pltpu.make_async_remote_copy(
            first, firsts.at[me], first_send, first_recv, device_id=d, device_id_type=MESH
        ).start()
    rows = pl.ds(pl.multiple_of(part * 8, 8), 8)
    for _, d in others:
        pltpu.make_async_remote_copy(
            tile, router.at[rows, mine], tile_send, tile_recv, device_id=d, device_id_type=MESH
        ).start()
    pltpu.make_async_copy(tile, router.at[rows, mine], own_sem.at[1]).start()

    @pl.loop(1, experts)
    def _(e):
        for t in range(2):
            chunk = t * experts + e
            top = largest(t, e)
            for k in range(strips):
                local[chunk, k : k + 1, :] = top[:, k * LANES : (k + 1) * LANES]
            owner = chunk
            home = (zl, x, owner // (ny * nc), lax.rem(owner // nc, ny), lax.rem(owner, nc))

            @pl.when(owner != me)
            def _():
                pltpu.make_async_remote_copy(
                    local.at[chunk], parts.at[me], part_send, part_recv,
                    device_id=home, device_id_type=MESH,
                ).start()

            @pl.when(owner == me)
            def _():
                parts[me] = local[chunk]

    def send(t, e):
        chunk = t * experts + e
        scale = scales[chunk]
        inverse = 1.0 / scale
        for k in range(strips):
            lanes = slice(k * LANES, (k + 1) * LANES)
            latest = train[t, e, :, lanes] + other[t, e, :, lanes].astype(jnp.float32)
            turned[t, lanes, :] = (latest * inverse[k : k + 1, :]).T
        for p in range(members):
            blocks[p, chunk] = turned[t, p * cut : (p + 1) * cut, :].astype(blocks.dtype)
        for p, d in others:
            pltpu.make_async_remote_copy(
                blocks.at[p, chunk], arrays[t][2].at[e, :, mine], send_sem, recv_sem,
                device_id=d, device_id_type=MESH,
            ).start()
        pltpu.make_async_copy(
            blocks.at[me, chunk], arrays[t][2].at[e, :, mine], own_sem.at[0]
        ).start()

    got = firsts.at[pl.ds(0, members - 1)]
    pltpu.make_async_copy(got, got, first_recv).wait()
    for t in range(2):
        scales[t * experts] = jnp.max(firsts[:, t], axis=0)
    send(0, 0)

    row = router.at[rows, pl.ds(0, (members - 1) * LANES)]
    pltpu.make_async_copy(row, row, tile_recv).wait()
    pltpu.make_async_copy(tile, router.at[rows, mine], own_sem.at[1]).wait()
    pltpu.make_async_remote_copy(
        router.at[rows], router.at[rows], pair_send, pair_recv, device_id=across, device_id_type=MESH
    ).start()

    owns = lax.rem(me, experts) != 0

    @pl.when(owns)
    def _():
        got = parts.at[pl.ds(0, members - 1)]
        pltpu.make_async_copy(got, got, part_recv).wait()
        scales[me] = jnp.max(parts[...], axis=0)
        for _, d in others:
            pltpu.make_async_remote_copy(
                scales.at[me], scales.at[me], scale_send, scale_recv.at[me],
                device_id=d, device_id_type=MESH,
            ).start()

    send(1, 0)

    pltpu.make_async_remote_copy(
        router.at[rows], router.at[rows], pair_send, pair_recv, device_id=across, device_id_type=MESH
    ).wait()
    for d in along:
        for h in range(nzl):
            block = pl.ds(pl.multiple_of((h * nx + x) * 8, 8), 8)
            pltpu.make_async_remote_copy(
                router.at[block], router.at[block], row_send, row_recv, device_id=d, device_id_type=MESH
            ).start()

    @pl.loop(1, experts)
    def _(e):
        for t in range(2):
            chunk = t * experts + e

            @pl.when(chunk != me)
            def _():
                pltpu.make_async_copy(
                    scales.at[chunk], scales.at[chunk], scale_recv.at[chunk]
                ).wait()

            send(t, e)

    for t, out in enumerate((sg, su)):
        whole = jnp.concatenate(
            [scales[t * experts : (t + 1) * experts, k, :] for k in range(strips)], axis=1
        )
        for p in range(members):

            @pl.when(me == p)
            def _(out=out, whole=whole, p=p):
                out[...] = whole[:, p * cut : (p + 1) * cut]

    def drain(ref, sem):
        pltpu.make_async_copy(ref, ref, sem).wait()

    drain(firsts.at[pl.ds(0, members - 1)], first_send)
    row = router.at[pl.ds(0, 8), pl.ds(0, (members - 1) * LANES)]
    drain(row, tile_send)

    @pl.when(owns)
    def _():
        drain(local.at[pl.ds(0, members - 3)], part_send)
        drain(firsts.at[pl.ds(0, members - 1), 0], scale_send)

    @pl.when(jnp.logical_not(owns))
    def _():
        drain(local.at[pl.ds(0, members - 2)], part_send)

    count = nzl * (nx - 1) * 8
    drain(router.at[pl.ds(0, count)], row_send)
    drain(router.at[pl.ds(0, count)], row_recv)
    drain(blocks.at[0], own_sem.at[0])
    drain(blocks.at[pl.ds(0, members - 1)], send_sem)
    drain(blocks.at[pl.ds(0, members - 1)], recv_sem)


def per_device(sizes, train_gate, other_gate, train_up, other_up, router_weight, router_gain):
    experts, depth, width = train_gate.shape
    members = sizes[2] * sizes[3] * sizes[4]
    parts = sizes[0] * sizes[1]
    cut = width // members
    strips = width // LANES
    chunks = 2 * experts
    dma, bf16, f32 = pltpu.SemaphoreType.DMA, jnp.bfloat16, jnp.float32
    hbm = pl.BlockSpec(memory_space=pl.ANY)
    vmem = pl.BlockSpec(memory_space=pltpu.VMEM)
    gate, up, sg, su, router = pl.pallas_call(
        functools.partial(kernel, sizes),
        out_shape=(
            jax.ShapeDtypeStruct((experts, cut, depth * members), bf16),
            jax.ShapeDtypeStruct((experts, cut, depth * members), bf16),
            jax.ShapeDtypeStruct((experts, cut), f32),
            jax.ShapeDtypeStruct((experts, cut), f32),
            jax.ShapeDtypeStruct((8 * parts, depth * members), bf16),
        ),
        in_specs=[hbm] * 4 + [vmem] * 2,
        out_specs=(hbm, hbm, vmem, vmem, hbm),
        scratch_shapes=[
            pltpu.VMEM((2, experts, depth, width), f32),
            pltpu.VMEM((2, experts, depth, width), bf16),
            pltpu.VMEM((2, width, depth), f32),
            pltpu.VMEM((members, chunks, cut, depth), bf16),
            pltpu.VMEM((2, strips, LANES), f32),
            pltpu.VMEM((members, 2, strips, LANES), f32),
            pltpu.VMEM((chunks, strips, LANES), f32),
            pltpu.VMEM((members, strips, LANES), f32),
            pltpu.VMEM((chunks, strips, LANES), f32),
            pltpu.VMEM((8, depth), bf16),
            dma((2, 2, experts)),
            dma, dma, dma((2,)),
            dma, dma, dma, dma, dma, dma((chunks,)),
            dma, dma, dma, dma, dma, dma,
        ],
        compiler_params=pltpu.CompilerParams(
            collective_id=0, has_side_effects=True, vmem_limit_bytes=40 * 2**20
        ),
        name="regroup",
    )(train_gate, other_gate, train_up, other_up, router_weight.T, router_gain[None])
    return gate.transpose(0, 2, 1), up.transpose(0, 2, 1), sg, su, router.T


def solution(mesh):
    sizes = (2, mesh.shape["ep"] // 2, 2, mesh.shape["fsdp"] // 4, 2)
    split = Mesh(mesh.devices.reshape(sizes), AXES)
    return jax.shard_map(
        functools.partial(per_device, sizes),
        mesh=split,
        in_specs=(
            P(EP, FSDP, None),
            P(EP, FSDP, None),
            P(EP, FSDP, None),
            P(EP, FSDP, None),
            P(FSDP, EP),
            P(FSDP),
        ),
        out_specs=(P(EP, None, FSDP), P(EP, None, FSDP), P(EP, FSDP), P(EP, FSDP), P()),
        check_vma=False,
    )
```

```python
import functools

import jax
import jax.numpy as jnp
from jax import lax
from jax.experimental import pallas as pl
from jax.experimental.pallas import tpu as pltpu
from jax.sharding import Mesh
from jax.sharding import PartitionSpec as P

MESH = pl.DeviceIdType.MESH
AXES = ("zl", "x", "zh", "y", "c")
EP = ("zl", "x")
FSDP = ("zh", "y", "c")
LANES = 128
PEERS = (
    (1, 1, 0), (3, 1, 0), (0, 1, 0), (2, 1, 0), (1, 0, 0), (3, 0, 0), (2, 0, 0),
    (1, 1, 1), (3, 1, 1), (0, 1, 1), (2, 1, 1), (1, 0, 1), (3, 0, 1), (2, 0, 1), (0, 0, 1),
)


def kernel(
    sizes,
    tg, og, tu, ou, rw, rg,
    gate, up, sg, su, router,
    train, other, turned, blocks, first, firsts, local, parts, scales, tiles, weight, gain,
    load_sem, small_sem, send_sem, recv_sem, own_sem,
    first_send, first_recv, part_send, part_recv, scale_send, scale_recv,
    tile_send, tile_recv, pair_send, pair_recv, row_send, row_recv,
):
    nzl, nx, nzh, ny, nc = sizes
    experts, depth, width = tg.shape
    members = nzh * ny * nc
    cut = width // members
    strips = width // LANES
    zl, x, zh, y, c = (lax.axis_index(a) for a in AXES)
    me = (zh * ny + y) * nc + c
    arrays = ((tg, og, gate), (tu, ou, up))

    def load(t, e):
        return (
            pltpu.make_async_copy(arrays[t][0].at[e], train.at[t, e], load_sem.at[0, t, e]),
            pltpu.make_async_copy(arrays[t][1].at[e], other.at[t, e], load_sem.at[1, t, e]),
        )

    def peer(step):
        dy, dz, dc = step
        ty, tz, tc = lax.rem(y + dy, ny), lax.rem(zh + dz, nzh), lax.rem(c + dc, nc)
        return (tz * ny + ty) * nc + tc, (zl, x, tz, ty, tc)

    others = [peer(step) for step in PEERS]
    across = (lax.rem(zl + 1, nzl), x, zh, y, c)
    along = [(zl, lax.rem(x + k, nx), zh, y, c) for k in range(1, nx)]
    mine = pl.ds(pl.multiple_of(me * LANES, LANES), LANES)

    barrier = pltpu.get_barrier_semaphore()
    everyone = [d for _, d in others] + [across] + along
    for d in everyone:
        pl.semaphore_signal(barrier, inc=1, device_id=d, device_id_type=MESH)

    for t in range(2):
        for copy in load(t, 0):
            copy.start()
    small = (
        pltpu.make_async_copy(rw, weight, small_sem.at[0]),
        pltpu.make_async_copy(rg, gain, small_sem.at[1]),
    )
    for copy in small:
        copy.start()

    @pl.loop(1, experts)
    def _(e):
        for t in range(2):
            for copy in load(t, e):
                copy.start()

    def largest(t, e):
        for copy in load(t, e):
            copy.wait()
        latest = train[t, e] + other[t, e].astype(jnp.float32)
        return jnp.max(jnp.abs(latest), axis=0, keepdims=True)

    for t in range(2):
        top = largest(t, 0)
        for k in range(strips):
            first[t, k : k + 1, :] = top[:, k * LANES : (k + 1) * LANES]
        firsts[t, me] = first[t]
    for copy in small:
        copy.wait()
    tiles[zl] = (weight[...] * gain[...]).astype(tiles.dtype)

    pl.semaphore_wait(barrier, len(everyone))
    for t in range(2):
        for _, d in others:
            pltpu.make_async_remote_copy(
                first.at[t], firsts.at[t, me], first_send.at[t], first_recv.at[t],
                device_id=d, device_id_type=MESH,
            ).start()
    handed = pltpu.make_async_remote_copy(
        tiles.at[zl], tiles.at[zl], pair_send, pair_recv, device_id=across, device_id_type=MESH
    )
    handed.start()

    def turn(t, e):
        for k in range(strips):
            lanes = slice(k * LANES, (k + 1) * LANES)
            latest = train[t, e, :, lanes] + other[t, e, :, lanes].astype(jnp.float32)
            turned[t, lanes, :] = latest.T

    turn(0, 0)

    @pl.loop(1, experts)
    def _(e):
        for t in range(2):
            chunk = t * experts + e
            top = largest(t, e)
            for k in range(strips):
                local[chunk, k : k + 1, :] = top[:, k * LANES : (k + 1) * LANES]
            owner = chunk
            home = (zl, x, owner // (ny * nc), lax.rem(owner // nc, ny), lax.rem(owner, nc))

            @pl.when(owner != me)
            def _():
                pltpu.make_async_remote_copy(
                    local.at[chunk], parts.at[me], part_send, part_recv,
                    device_id=home, device_id_type=MESH,
                ).start()

            @pl.when(owner == me)
            def _():
                parts[me] = local[chunk]

    def deliver(t, e):
        chunk = t * experts + e
        for p, d in others:
            pltpu.make_async_remote_copy(
                blocks.at[p, chunk], arrays[t][2].at[e, :, mine], send_sem, recv_sem,
                device_id=d, device_id_type=MESH,
            ).start()
        pltpu.make_async_copy(
            blocks.at[me, chunk], arrays[t][2].at[e, :, mine], own_sem.at[0]
        ).start()

    def send(t, e):
        chunk = t * experts + e
        inverse = 1.0 / scales[chunk]
        for k in range(strips):
            lanes = slice(k * LANES, (k + 1) * LANES)
            latest = train[t, e, :, lanes] + other[t, e, :, lanes].astype(jnp.float32)
            turned[t, lanes, :] = (latest * inverse[k : k + 1, :]).T
        for p in range(members):
            blocks[p, chunk] = turned[t, p * cut : (p + 1) * cut, :].astype(blocks.dtype)
        deliver(t, e)

    def send_first(t):
        got = firsts.at[t, pl.ds(0, members - 1)]
        pltpu.make_async_copy(got, got, first_recv.at[t]).wait()
        scale = jnp.max(firsts[t], axis=0)
        scales[t * experts] = scale
        inverse = (1.0 / scale).T
        for p in range(members):
            pieces, row = [], p * cut
            while row < (p + 1) * cut:
                k = row // LANES
                end = min((k + 1) * LANES, (p + 1) * cut)
                column = inverse[row - k * LANES : end - k * LANES, k : k + 1]
                pieces.append(turned[t, row:end, :] * column)
                row = end
            blocks[p, t * experts] = jnp.concatenate(pieces, axis=0).astype(blocks.dtype)
        deliver(t, 0)

    handed.wait()
    bands = [pl.ds(pl.multiple_of((h * nx + x) * 8, 8), 8) for h in range(nzl)]
    for _, d in others:
        for h, band in enumerate(bands):
            pltpu.make_async_remote_copy(
                tiles.at[h], router.at[band, mine], tile_send, tile_recv,
                device_id=d, device_id_type=MESH,
            ).start()
    kept = [
        pltpu.make_async_copy(tiles.at[h], router.at[band, mine], own_sem.at[1 + h])
        for h, band in enumerate(bands)
    ]
    for copy in kept:
        copy.start()
    turn(1, 0)

    send_first(0)

    owns = lax.rem(me, experts) != 0

    @pl.when(owns)
    def _():
        got = parts.at[pl.ds(0, members - 1)]
        pltpu.make_async_copy(got, got, part_recv).wait()
        scales[me] = jnp.max(parts[...], axis=0)
        for _, d in others:
            pltpu.make_async_remote_copy(
                scales.at[me], scales.at[me], scale_send, scale_recv.at[me],
                device_id=d, device_id_type=MESH,
            ).start()

    send_first(1)

    for copy in kept:
        copy.wait()
    row = router.at[pl.ds(0, nzl * 8), pl.ds(0, (members - 1) * LANES)]
    pltpu.make_async_copy(row, row, tile_recv).wait()
    for d in along:
        for band in bands:
            pltpu.make_async_remote_copy(
                router.at[band], router.at[band], row_send, row_recv, device_id=d, device_id_type=MESH
            ).start()

    @pl.loop(1, experts)
    def _(e):
        for t in range(2):
            chunk = t * experts + e

            @pl.when(chunk != me)
            def _():
                pltpu.make_async_copy(
                    scales.at[chunk], scales.at[chunk], scale_recv.at[chunk]
                ).wait()

            send(t, e)

    for t, out in enumerate((sg, su)):
        whole = jnp.concatenate(
            [scales[t * experts : (t + 1) * experts, k, :] for k in range(strips)], axis=1
        )
        for p in range(members):

            @pl.when(me == p)
            def _(out=out, whole=whole, p=p):
                out[...] = whole[:, p * cut : (p + 1) * cut]

    def drain(ref, sem):
        pltpu.make_async_copy(ref, ref, sem).wait()

    for t in range(2):
        drain(firsts.at[t, pl.ds(0, members - 1)], first_send.at[t])
    drain(row, tile_send)

    @pl.when(owns)
    def _():
        drain(local.at[pl.ds(0, members - 3)], part_send)
        drain(firsts.at[0, pl.ds(0, members - 1)], scale_send)

    @pl.when(jnp.logical_not(owns))
    def _():
        drain(local.at[pl.ds(0, members - 2)], part_send)

    count = nzl * (nx - 1) * 8
    drain(router.at[pl.ds(0, count)], row_send)
    drain(router.at[pl.ds(0, count)], row_recv)
    drain(blocks.at[0], own_sem.at[0])
    drain(blocks.at[pl.ds(0, members - 1)], send_sem)
    drain(blocks.at[pl.ds(0, members - 1)], recv_sem)


def finish(*refs):
    n = len(refs) // 2
    arrived, outs, sem = refs[:n], refs[n:-1], refs[-1]
    copies = []
    for source, out in zip(arrived, outs):
        if len(source.shape) == 3:
            pieces = [(source.at[e], out.at[e]) for e in range(source.shape[0])]
        else:
            pieces = [(source, out)]
        copies += [
            pltpu.make_async_copy(a, b, sem.at[len(copies) + k]) for k, (a, b) in enumerate(pieces)
        ]
    for copy in copies:
        copy.start()
    for copy in copies:
        copy.wait()


def per_device(sizes, train_gate, other_gate, train_up, other_up, router_weight, router_gain):
    experts, depth, width = train_gate.shape
    members = sizes[2] * sizes[3] * sizes[4]
    parts = sizes[0] * sizes[1]
    cut = width // members
    strips = width // LANES
    chunks = 2 * experts
    dma, bf16, f32 = pltpu.SemaphoreType.DMA, jnp.bfloat16, jnp.float32
    hbm = pl.BlockSpec(memory_space=pltpu.HBM)
    vmem = pl.BlockSpec(memory_space=pltpu.VMEM)
    shapes = (
        ((experts, cut, depth * members), bf16),
        ((experts, cut, depth * members), bf16),
        ((experts, cut), f32),
        ((experts, cut), f32),
        ((8 * parts, depth * members), bf16),
    )
    operands = (train_gate, other_gate, train_up, other_up, router_weight.T, router_gain[None])
    arrived = pl.pallas_call(
        functools.partial(kernel, sizes),
        out_shape=[pltpu.VMEM(*shape) for shape in shapes],
        in_specs=[hbm] * 6,
        out_specs=[vmem] * 5,
        scratch_shapes=[
            pltpu.VMEM((2, experts, depth, width), f32),
            pltpu.VMEM((2, experts, depth, width), bf16),
            pltpu.VMEM((2, width, depth), f32),
            pltpu.VMEM((members, chunks, cut, depth), bf16),
            pltpu.VMEM((2, strips, LANES), f32),
            pltpu.VMEM((2, members, strips, LANES), f32),
            pltpu.VMEM((chunks, strips, LANES), f32),
            pltpu.VMEM((members, strips, LANES), f32),
            pltpu.VMEM((chunks, strips, LANES), f32),
            pltpu.VMEM((sizes[0], 8, depth), bf16),
            pltpu.VMEM((8, depth), f32),
            pltpu.VMEM((1, depth), f32),
            dma((2, 2, experts)), dma((2,)),
            dma, dma, dma((1 + sizes[0],)),
            dma((2,)), dma((2,)), dma, dma, dma, dma((chunks,)),
            dma, dma, dma, dma, dma, dma,
        ],
        compiler_params=pltpu.CompilerParams(
            collective_id=0, has_side_effects=True, vmem_limit_bytes=48 * 2**20
        ),
        name="regroup",
    )(*(pltpu.with_memory_space_constraint(a, pltpu.HBM) for a in operands))
    gate, up, sg, su, router = pl.pallas_call(
        finish,
        out_shape=[jax.ShapeDtypeStruct(*shape) for shape in shapes],
        in_specs=[vmem] * 5,
        out_specs=[hbm] * 5,
        scratch_shapes=[dma((2 * experts + 3,))],
        compiler_params=pltpu.CompilerParams(vmem_limit_bytes=4 * 2**20),
        name="finish",
    )(*(pltpu.with_memory_space_constraint(a, pltpu.VMEM) for a in arrived))
    return gate.transpose(0, 2, 1), up.transpose(0, 2, 1), sg, su, router.T


def solution(mesh):
    sizes = (2, mesh.shape["ep"] // 2, 2, mesh.shape["fsdp"] // 4, 2)
    split = Mesh(mesh.devices.reshape(sizes), AXES)
    return jax.shard_map(
        functools.partial(per_device, sizes),
        mesh=split,
        in_specs=(
            P(EP, FSDP, None),
            P(EP, FSDP, None),
            P(EP, FSDP, None),
            P(EP, FSDP, None),
            P(FSDP, EP),
            P(FSDP),
        ),
        out_specs=(P(EP, None, FSDP), P(EP, None, FSDP), P(EP, FSDP), P(EP, FSDP), P()),
        check_vma=False,
    )
```

```python
import functools

import jax
import jax.numpy as jnp
from jax import lax
from jax.experimental import pallas as pl
from jax.experimental.pallas import tpu as pltpu
from jax.sharding import Mesh
from jax.sharding import PartitionSpec as P

MESH = pl.DeviceIdType.MESH
AXES = ("zl", "x", "zh", "y", "c")
EP = ("zl", "x")
FSDP = ("zh", "y", "c")
LANES = 128
PEERS = (
    (2, 1, 1), (2, 1, 0), (1, 1, 1), (1, 1, 0), (3, 1, 1), (3, 1, 0), (0, 1, 1), (0, 1, 0),
    (2, 0, 1), (2, 0, 0), (1, 0, 1), (1, 0, 0), (3, 0, 1), (3, 0, 0), (0, 0, 1),
)


def kernel(
    sizes,
    tg, og, tu, ou, rw, rg,
    gate, up, sg, su, router,
    train, other, turned, blocks, first, firsts, local, parts, scales, tiles, weight, gain,
    load_sem, small_sem, send_sem, recv_sem, own_sem,
    first_send, first_recv, part_send, part_recv, scale_send, scale_recv,
    tile_send, tile_recv, pair_send, pair_recv, row_send, row_recv,
):
    nzl, nx, nzh, ny, nc = sizes
    experts, depth, width = tg.shape
    members = nzh * ny * nc
    cut = width // members
    strips = width // LANES
    zl, x, zh, y, c = (lax.axis_index(a) for a in AXES)
    me = (zh * ny + y) * nc + c
    arrays = ((tg, og, gate), (tu, ou, up))

    def load(t, e):
        return (
            pltpu.make_async_copy(arrays[t][0].at[e], train.at[t, e], load_sem.at[0, t, e]),
            pltpu.make_async_copy(arrays[t][1].at[e], other.at[t, e], load_sem.at[1, t, e]),
        )

    def peer(step):
        dy, dz, dc = step
        ty, tz, tc = lax.rem(y + dy, ny), lax.rem(zh + dz, nzh), lax.rem(c + dc, nc)
        return (tz * ny + ty) * nc + tc, (zl, x, tz, ty, tc)

    others = [peer(step) for step in PEERS]
    across = (lax.rem(zl + 1, nzl), x, zh, y, c)
    along = [(zl, lax.rem(x + k, nx), zh, y, c) for k in range(1, nx)]
    mine = pl.ds(pl.multiple_of(me * LANES, LANES), LANES)

    barrier = pltpu.get_barrier_semaphore()
    everyone = [d for _, d in others] + [across] + along
    for d in everyone:
        pl.semaphore_signal(barrier, inc=1, device_id=d, device_id_type=MESH)

    for t in range(2):
        for copy in load(t, 0):
            copy.start()
    small = (
        pltpu.make_async_copy(rw, weight, small_sem.at[0]),
        pltpu.make_async_copy(rg, gain, small_sem.at[1]),
    )
    for copy in small:
        copy.start()

    @pl.loop(1, experts)
    def _(e):
        for t in range(2):
            for copy in load(t, e):
                copy.start()

    def largest(t, e):
        for copy in load(t, e):
            copy.wait()
        latest = train[t, e] + other[t, e].astype(jnp.float32)
        return jnp.max(jnp.abs(latest), axis=0, keepdims=True)

    for t in range(2):
        top = largest(t, 0)
        for k in range(strips):
            first[t, k : k + 1, :] = top[:, k * LANES : (k + 1) * LANES]
        firsts[t, me] = first[t]
    for copy in small:
        copy.wait()
    tiles[zl] = (weight[...] * gain[...]).astype(tiles.dtype)

    pl.semaphore_wait(barrier, len(everyone))
    for t in range(2):
        for _, d in others:
            pltpu.make_async_remote_copy(
                first.at[t], firsts.at[t, me], first_send.at[t], first_recv.at[t],
                device_id=d, device_id_type=MESH,
            ).start()
    handed = pltpu.make_async_remote_copy(
        tiles.at[zl], tiles.at[zl], pair_send, pair_recv, device_id=across, device_id_type=MESH
    )
    handed.start()

    def turn(t, e):
        for k in range(strips):
            lanes = slice(k * LANES, (k + 1) * LANES)
            latest = train[t, e, :, lanes] + other[t, e, :, lanes].astype(jnp.float32)
            turned[t, lanes, :] = latest.T

    turn(0, 0)

    @pl.loop(1, experts)
    def _(e):
        for t in range(2):
            chunk = t * experts + e
            top = largest(t, e)
            for k in range(strips):
                local[chunk, k : k + 1, :] = top[:, k * LANES : (k + 1) * LANES]
            owner = chunk
            home = (zl, x, owner // (ny * nc), lax.rem(owner // nc, ny), lax.rem(owner, nc))

            @pl.when(owner != me)
            def _():
                pltpu.make_async_remote_copy(
                    local.at[chunk], parts.at[me], part_send, part_recv,
                    device_id=home, device_id_type=MESH,
                ).start()

            @pl.when(owner == me)
            def _():
                parts[me] = local[chunk]

    def deliver(t, e):
        chunk = t * experts + e
        for p, d in others:
            pltpu.make_async_remote_copy(
                blocks.at[p, chunk], arrays[t][2].at[e, :, mine], send_sem, recv_sem,
                device_id=d, device_id_type=MESH,
            ).start()
        pltpu.make_async_copy(
            blocks.at[me, chunk], arrays[t][2].at[e, :, mine], own_sem.at[0]
        ).start()

    def send(t, e):
        chunk = t * experts + e
        inverse = 1.0 / scales[chunk]
        for k in range(strips):
            lanes = slice(k * LANES, (k + 1) * LANES)
            latest = train[t, e, :, lanes] + other[t, e, :, lanes].astype(jnp.float32)
            turned[t, lanes, :] = (latest * inverse[k : k + 1, :]).T
        for p in range(members):
            blocks[p, chunk] = turned[t, p * cut : (p + 1) * cut, :].astype(blocks.dtype)
        deliver(t, e)

    def send_first(t):
        got = firsts.at[t, pl.ds(0, members - 1)]
        pltpu.make_async_copy(got, got, first_recv.at[t]).wait()
        scale = jnp.max(firsts[t], axis=0)
        scales[t * experts] = scale
        inverse = (1.0 / scale).T
        for p in range(members):
            pieces, row = [], p * cut
            while row < (p + 1) * cut:
                k = row // LANES
                end = min((k + 1) * LANES, (p + 1) * cut)
                column = inverse[row - k * LANES : end - k * LANES, k : k + 1]
                pieces.append(turned[t, row:end, :] * column)
                row = end
            blocks[p, t * experts] = jnp.concatenate(pieces, axis=0).astype(blocks.dtype)
        deliver(t, 0)

    handed.wait()
    bands = [pl.ds(pl.multiple_of((h * nx + x) * 8, 8), 8) for h in range(nzl)]
    for _, d in others:
        for h, band in enumerate(bands):
            pltpu.make_async_remote_copy(
                tiles.at[h], router.at[band, mine], tile_send, tile_recv,
                device_id=d, device_id_type=MESH,
            ).start()
    kept = [
        pltpu.make_async_copy(tiles.at[h], router.at[band, mine], own_sem.at[1 + h])
        for h, band in enumerate(bands)
    ]
    for copy in kept:
        copy.start()
    turn(1, 0)

    send_first(0)

    owns = lax.rem(me, experts) != 0

    @pl.when(owns)
    def _():
        got = parts.at[pl.ds(0, members - 1)]
        pltpu.make_async_copy(got, got, part_recv).wait()
        scales[me] = jnp.max(parts[...], axis=0)
        for _, d in others:
            pltpu.make_async_remote_copy(
                scales.at[me], scales.at[me], scale_send, scale_recv.at[me],
                device_id=d, device_id_type=MESH,
            ).start()

    send_first(1)

    for copy in kept:
        copy.wait()
    row = router.at[pl.ds(0, nzl * 8), pl.ds(0, (members - 1) * LANES)]
    pltpu.make_async_copy(row, row, tile_recv).wait()
    for d in along:
        for band in bands:
            pltpu.make_async_remote_copy(
                router.at[band], router.at[band], row_send, row_recv, device_id=d, device_id_type=MESH
            ).start()

    @pl.loop(1, experts)
    def _(e):
        for t in range(2):
            chunk = t * experts + e

            @pl.when(chunk != me)
            def _():
                pltpu.make_async_copy(
                    scales.at[chunk], scales.at[chunk], scale_recv.at[chunk]
                ).wait()

            send(t, e)

    for t, out in enumerate((sg, su)):
        whole = jnp.concatenate(
            [scales[t * experts : (t + 1) * experts, k, :] for k in range(strips)], axis=1
        )
        for p in range(members):

            @pl.when(me == p)
            def _(out=out, whole=whole, p=p):
                out[...] = whole[:, p * cut : (p + 1) * cut]

    def drain(ref, sem):
        pltpu.make_async_copy(ref, ref, sem).wait()

    for t in range(2):
        drain(firsts.at[t, pl.ds(0, members - 1)], first_send.at[t])
    drain(row, tile_send)

    @pl.when(owns)
    def _():
        drain(local.at[pl.ds(0, members - 3)], part_send)
        drain(firsts.at[0, pl.ds(0, members - 1)], scale_send)

    @pl.when(jnp.logical_not(owns))
    def _():
        drain(local.at[pl.ds(0, members - 2)], part_send)

    count = nzl * (nx - 1) * 8
    drain(router.at[pl.ds(0, count)], row_send)
    drain(router.at[pl.ds(0, count)], row_recv)
    drain(blocks.at[0], own_sem.at[0])
    drain(blocks.at[pl.ds(0, members - 1)], send_sem)
    drain(blocks.at[pl.ds(0, members - 1)], recv_sem)


def finish(*refs):
    n = len(refs) // 2
    arrived, outs, sem = refs[:n], refs[n:-1], refs[-1]
    copies = []
    for source, out in zip(arrived, outs):
        if len(source.shape) == 3:
            pieces = [(source.at[e], out.at[e]) for e in range(source.shape[0])]
        else:
            pieces = [(source, out)]
        copies += [
            pltpu.make_async_copy(a, b, sem.at[len(copies) + k]) for k, (a, b) in enumerate(pieces)
        ]
    for copy in copies:
        copy.start()
    for copy in copies:
        copy.wait()


def per_device(sizes, train_gate, other_gate, train_up, other_up, router_weight, router_gain):
    experts, depth, width = train_gate.shape
    members = sizes[2] * sizes[3] * sizes[4]
    parts = sizes[0] * sizes[1]
    cut = width // members
    strips = width // LANES
    chunks = 2 * experts
    dma, bf16, f32 = pltpu.SemaphoreType.DMA, jnp.bfloat16, jnp.float32
    hbm = pl.BlockSpec(memory_space=pltpu.HBM)
    vmem = pl.BlockSpec(memory_space=pltpu.VMEM)
    shapes = (
        ((experts, cut, depth * members), bf16),
        ((experts, cut, depth * members), bf16),
        ((experts, cut), f32),
        ((experts, cut), f32),
        ((8 * parts, depth * members), bf16),
    )
    operands = (train_gate, other_gate, train_up, other_up, router_weight.T, router_gain[None])
    arrived = pl.pallas_call(
        functools.partial(kernel, sizes),
        out_shape=[pltpu.VMEM(*shape) for shape in shapes],
        in_specs=[hbm] * 6,
        out_specs=[vmem] * 5,
        scratch_shapes=[
            pltpu.VMEM((2, experts, depth, width), f32),
            pltpu.VMEM((2, experts, depth, width), bf16),
            pltpu.VMEM((2, width, depth), f32),
            pltpu.VMEM((members, chunks, cut, depth), bf16),
            pltpu.VMEM((2, strips, LANES), f32),
            pltpu.VMEM((2, members, strips, LANES), f32),
            pltpu.VMEM((chunks, strips, LANES), f32),
            pltpu.VMEM((members, strips, LANES), f32),
            pltpu.VMEM((chunks, strips, LANES), f32),
            pltpu.VMEM((sizes[0], 8, depth), bf16),
            pltpu.VMEM((8, depth), f32),
            pltpu.VMEM((1, depth), f32),
            dma((2, 2, experts)), dma((2,)),
            dma, dma, dma((1 + sizes[0],)),
            dma((2,)), dma((2,)), dma, dma, dma, dma((chunks,)),
            dma, dma, dma, dma, dma, dma,
        ],
        compiler_params=pltpu.CompilerParams(
            collective_id=0, has_side_effects=True, vmem_limit_bytes=48 * 2**20
        ),
        name="regroup",
    )(*(pltpu.with_memory_space_constraint(a, pltpu.HBM) for a in operands))
    gate, up, sg, su, router = pl.pallas_call(
        finish,
        out_shape=[jax.ShapeDtypeStruct(*shape) for shape in shapes],
        in_specs=[vmem] * 5,
        out_specs=[hbm] * 5,
        scratch_shapes=[dma((2 * experts + 3,))],
        compiler_params=pltpu.CompilerParams(vmem_limit_bytes=4 * 2**20),
        name="finish",
    )(*(pltpu.with_memory_space_constraint(a, pltpu.VMEM) for a in arrived))
    return gate.transpose(0, 2, 1), up.transpose(0, 2, 1), sg, su, router.T


def solution(mesh):
    sizes = (2, mesh.shape["ep"] // 2, 2, mesh.shape["fsdp"] // 4, 2)
    split = Mesh(mesh.devices.reshape(sizes), AXES)
    return jax.shard_map(
        functools.partial(per_device, sizes),
        mesh=split,
        in_specs=(
            P(EP, FSDP, None),
            P(EP, FSDP, None),
            P(EP, FSDP, None),
            P(EP, FSDP, None),
            P(FSDP, EP),
            P(FSDP),
        ),
        out_specs=(P(EP, None, FSDP), P(EP, None, FSDP), P(EP, FSDP), P(EP, FSDP), P()),
        check_vma=False,
    )
```

```python
import functools

import jax
import jax.numpy as jnp
from jax import lax
from jax.experimental import pallas as pl
from jax.experimental.pallas import tpu as pltpu
from jax.sharding import Mesh
from jax.sharding import PartitionSpec as P

MESH = pl.DeviceIdType.MESH
AXES = ("zl", "x", "zh", "y", "c")
EP = ("zl", "x")
FSDP = ("zh", "y", "c")
LANES = 128
PEERS = (
    (2, 1, 1), (2, 1, 0), (1, 1, 1), (1, 1, 0), (3, 1, 1), (3, 1, 0), (0, 1, 1), (0, 1, 0),
    (2, 0, 1), (2, 0, 0), (1, 0, 1), (1, 0, 0), (3, 0, 1), (3, 0, 0), (0, 0, 1),
)


def kernel(
    sizes,
    tg, og, tu, ou, rw, rg,
    gate, up, sg, su, router,
    train, other, turned, blocks, first, firsts, local, parts, scales, tiles, weight, gain,
    load_sem, small_sem, send_sem, recv_sem, own_sem,
    first_send, first_recv, part_send, part_recv, scale_send, scale_recv, hand_send,
    tile_send, tile_recv, pair_send, pair_recv, row_send, row_recv,
):
    nzl, nx, nzh, ny, nc = sizes
    experts, depth, width = tg.shape
    members = nzh * ny * nc
    cut = width // members
    strips = width // LANES
    zl, x, zh, y, c = (lax.axis_index(a) for a in AXES)
    me = (zh * ny + y) * nc + c
    arrays = ((tg, og, gate), (tu, ou, up))

    def load(t, e):
        return (
            pltpu.make_async_copy(arrays[t][0].at[e], train.at[t, e], load_sem.at[0, t, e]),
            pltpu.make_async_copy(arrays[t][1].at[e], other.at[t, e], load_sem.at[1, t, e]),
        )

    def peer(step):
        dy, dz, dc = step
        ty, tz, tc = lax.rem(y + dy, ny), lax.rem(zh + dz, nzh), lax.rem(c + dc, nc)
        return (tz * ny + ty) * nc + tc, (zl, x, tz, ty, tc)

    others = [peer(step) for step in PEERS]
    across = (lax.rem(zl + 1, nzl), x, zh, y, c)
    along = [(zl, lax.rem(x + k, nx), zh, y, c) for k in range(1, nx)]
    mine = pl.ds(pl.multiple_of(me * LANES, LANES), LANES)

    barrier = pltpu.get_barrier_semaphore()
    everyone = [d for _, d in others] + [across] + along
    for d in everyone:
        pl.semaphore_signal(barrier, inc=1, device_id=d, device_id_type=MESH)

    for t in range(2):
        for copy in load(t, 0):
            copy.start()
    small = (
        pltpu.make_async_copy(rw, weight, small_sem.at[0]),
        pltpu.make_async_copy(rg, gain, small_sem.at[1]),
    )
    for copy in small:
        copy.start()

    @pl.loop(1, experts)
    def _(e):
        for t in range(2):
            for copy in load(t, e):
                copy.start()

    def largest(t, e):
        for copy in load(t, e):
            copy.wait()
        latest = train[t, e] + other[t, e].astype(jnp.float32)
        return jnp.max(jnp.abs(latest), axis=0, keepdims=True)

    for t in range(2):
        top = largest(t, 0)
        for k in range(strips):
            first[t, k : k + 1, :] = top[:, k * LANES : (k + 1) * LANES]
        firsts[t, me] = first[t]
    for copy in small:
        copy.wait()
    tiles[zl] = (weight[...] * gain[...]).astype(tiles.dtype)

    pl.semaphore_wait(barrier, len(everyone))
    for t in range(2):
        for _, d in others:
            pltpu.make_async_remote_copy(
                first.at[t], firsts.at[t, me], first_send.at[t], first_recv.at[t],
                device_id=d, device_id_type=MESH,
            ).start()
    handed = pltpu.make_async_remote_copy(
        tiles.at[zl], tiles.at[zl], pair_send, pair_recv, device_id=across, device_id_type=MESH
    )
    handed.start()

    def turn(t, e):
        for k in range(strips):
            lanes = slice(k * LANES, (k + 1) * LANES)
            latest = train[t, e, :, lanes] + other[t, e, :, lanes].astype(jnp.float32)
            turned[t, lanes, :] = latest.T

    turn(0, 0)

    @pl.loop(1, experts)
    def _(e):
        for t in range(2):
            chunk = t * experts + e
            top = largest(t, e)
            for k in range(strips):
                local[chunk, k : k + 1, :] = top[:, k * LANES : (k + 1) * LANES]
            owner = chunk
            home = (zl, x, owner // (ny * nc), lax.rem(owner // nc, ny), lax.rem(owner, nc))

            @pl.when(owner != me)
            def _():
                pltpu.make_async_remote_copy(
                    local.at[chunk], parts.at[me], part_send, part_recv,
                    device_id=home, device_id_type=MESH,
                ).start()

            @pl.when(owner == me)
            def _():
                parts[me] = local[chunk]

    def deliver(t, e):
        chunk = t * experts + e
        for p, d in others:
            pltpu.make_async_remote_copy(
                blocks.at[p, chunk], arrays[t][2].at[e, :, mine], send_sem, recv_sem,
                device_id=d, device_id_type=MESH,
            ).start()
        pltpu.make_async_copy(
            blocks.at[me, chunk], arrays[t][2].at[e, :, mine], own_sem.at[0]
        ).start()

    def send(t, e):
        chunk = t * experts + e
        inverse = 1.0 / scales[chunk]
        for k in range(strips):
            lanes = slice(k * LANES, (k + 1) * LANES)
            latest = train[t, e, :, lanes] + other[t, e, :, lanes].astype(jnp.float32)
            turned[t, lanes, :] = (latest * inverse[k : k + 1, :]).T
        for p in range(members):
            blocks[p, chunk] = turned[t, p * cut : (p + 1) * cut, :].astype(blocks.dtype)
        deliver(t, e)

    def send_first(t):
        got = firsts.at[t, pl.ds(0, members - 1)]
        pltpu.make_async_copy(got, got, first_recv.at[t]).wait()
        scale = jnp.max(firsts[t], axis=0)
        scales[t * experts] = scale
        inverse = (1.0 / scale).T
        for p in range(members):
            pieces, row = [], p * cut
            while row < (p + 1) * cut:
                k = row // LANES
                end = min((k + 1) * LANES, (p + 1) * cut)
                column = inverse[row - k * LANES : end - k * LANES, k : k + 1]
                pieces.append(turned[t, row:end, :] * column)
                row = end
            blocks[p, t * experts] = jnp.concatenate(pieces, axis=0).astype(blocks.dtype)
        deliver(t, 0)

    handed.wait()
    bands = [pl.ds(pl.multiple_of((h * nx + x) * 8, 8), 8) for h in range(nzl)]
    for _, d in others:
        for h, band in enumerate(bands):
            pltpu.make_async_remote_copy(
                tiles.at[h], router.at[band, mine], tile_send, tile_recv,
                device_id=d, device_id_type=MESH,
            ).start()
    kept = [
        pltpu.make_async_copy(tiles.at[h], router.at[band, mine], own_sem.at[1 + h])
        for h, band in enumerate(bands)
    ]
    for copy in kept:
        copy.start()
    send_first(0)
    turn(1, 0)

    owns = lax.rem(me, experts) != 0

    @pl.when(owns)
    def _():
        got = parts.at[pl.ds(0, members - 1)]
        pltpu.make_async_copy(got, got, part_recv).wait()
        scales[me] = jnp.max(parts[...], axis=0)
        for (_, d), step in zip(others, PEERS):
            if step[2] == 0 or step == PEERS[-1]:
                pltpu.make_async_remote_copy(
                    scales.at[me], scales.at[me], scale_send, scale_recv.at[me],
                    device_id=d, device_id_type=MESH,
                ).start()

    send_first(1)

    for copy in kept:
        copy.wait()
    row = router.at[pl.ds(0, nzl * 8), pl.ds(0, (members - 1) * LANES)]
    pltpu.make_async_copy(row, row, tile_recv).wait()
    for d in along:
        for band in bands:
            pltpu.make_async_remote_copy(
                router.at[band], router.at[band], row_send, row_recv, device_id=d, device_id_type=MESH
            ).start()

    mate = others[-1][1]

    @pl.loop(1, experts)
    def _(e):
        for t in range(2):
            chunk = t * experts + e

            @pl.when(chunk != me)
            def _():
                pltpu.make_async_copy(
                    scales.at[chunk], scales.at[chunk], scale_recv.at[chunk]
                ).wait()

                @pl.when(lax.rem(chunk, nc) == c)
                def _():
                    pltpu.make_async_remote_copy(
                        scales.at[chunk], scales.at[chunk], hand_send, scale_recv.at[chunk],
                        device_id=mate, device_id_type=MESH,
                    ).start()

            send(t, e)

    for t, out in enumerate((sg, su)):
        whole = jnp.concatenate(
            [scales[t * experts : (t + 1) * experts, k, :] for k in range(strips)], axis=1
        )
        for p in range(members):

            @pl.when(me == p)
            def _(out=out, whole=whole, p=p):
                out[...] = whole[:, p * cut : (p + 1) * cut]

    def drain(ref, sem):
        pltpu.make_async_copy(ref, ref, sem).wait()

    for t in range(2):
        drain(firsts.at[t, pl.ds(0, members - 1)], first_send.at[t])
    drain(row, tile_send)

    @pl.when(owns)
    def _():
        drain(local.at[pl.ds(0, members - 3)], part_send)
        drain(firsts.at[0, pl.ds(0, members // nc)], scale_send)

    @pl.when(jnp.logical_not(owns))
    def _():
        drain(local.at[pl.ds(0, members - 2)], part_send)

    for k in range(nc):
        handed_on = 2 * len([e for e in range(1, experts) if e % nc == k])
        for less in range(2):

            @pl.when(jnp.logical_and(c == k, owns == (less == 1)))
            def _(rows=handed_on - less):
                drain(local.at[pl.ds(0, rows)], hand_send)

    count = nzl * (nx - 1) * 8
    drain(router.at[pl.ds(0, count)], row_send)
    drain(router.at[pl.ds(0, count)], row_recv)
    drain(blocks.at[0], own_sem.at[0])
    drain(blocks.at[pl.ds(0, members - 1)], send_sem)
    drain(blocks.at[pl.ds(0, members - 1)], recv_sem)


def finish(*refs):
    n = len(refs) // 2
    arrived, outs, sem = refs[:n], refs[n:-1], refs[-1]
    copies = []
    for source, out in zip(arrived, outs):
        if len(source.shape) == 3:
            pieces = [(source.at[e], out.at[e]) for e in range(source.shape[0])]
        else:
            pieces = [(source, out)]
        copies += [
            pltpu.make_async_copy(a, b, sem.at[len(copies) + k]) for k, (a, b) in enumerate(pieces)
        ]
    for copy in copies:
        copy.start()
    for copy in copies:
        copy.wait()


def per_device(sizes, train_gate, other_gate, train_up, other_up, router_weight, router_gain):
    experts, depth, width = train_gate.shape
    members = sizes[2] * sizes[3] * sizes[4]
    parts = sizes[0] * sizes[1]
    cut = width // members
    strips = width // LANES
    chunks = 2 * experts
    dma, bf16, f32 = pltpu.SemaphoreType.DMA, jnp.bfloat16, jnp.float32
    hbm = pl.BlockSpec(memory_space=pltpu.HBM)
    vmem = pl.BlockSpec(memory_space=pltpu.VMEM)
    shapes = (
        ((experts, cut, depth * members), bf16),
        ((experts, cut, depth * members), bf16),
        ((experts, cut), f32),
        ((experts, cut), f32),
        ((8 * parts, depth * members), bf16),
    )
    operands = (train_gate, other_gate, train_up, other_up, router_weight.T, router_gain[None])
    arrived = pl.pallas_call(
        functools.partial(kernel, sizes),
        out_shape=[pltpu.VMEM(*shape) for shape in shapes],
        in_specs=[hbm] * 6,
        out_specs=[vmem] * 5,
        scratch_shapes=[
            pltpu.VMEM((2, experts, depth, width), f32),
            pltpu.VMEM((2, experts, depth, width), bf16),
            pltpu.VMEM((2, width, depth), f32),
            pltpu.VMEM((members, chunks, cut, depth), bf16),
            pltpu.VMEM((2, strips, LANES), f32),
            pltpu.VMEM((2, members, strips, LANES), f32),
            pltpu.VMEM((chunks, strips, LANES), f32),
            pltpu.VMEM((members, strips, LANES), f32),
            pltpu.VMEM((chunks, strips, LANES), f32),
            pltpu.VMEM((sizes[0], 8, depth), bf16),
            pltpu.VMEM((8, depth), f32),
            pltpu.VMEM((1, depth), f32),
            dma((2, 2, experts)), dma((2,)),
            dma, dma, dma((1 + sizes[0],)),
            dma((2,)), dma((2,)), dma, dma, dma, dma((chunks,)), dma,
            dma, dma, dma, dma, dma, dma,
        ],
        compiler_params=pltpu.CompilerParams(
            collective_id=0, has_side_effects=True, vmem_limit_bytes=48 * 2**20
        ),
        name="regroup",
    )(*(pltpu.with_memory_space_constraint(a, pltpu.HBM) for a in operands))
    gate, up, sg, su, router = pl.pallas_call(
        finish,
        out_shape=[jax.ShapeDtypeStruct(*shape) for shape in shapes],
        in_specs=[vmem] * 5,
        out_specs=[hbm] * 5,
        scratch_shapes=[dma((2 * experts + 3,))],
        compiler_params=pltpu.CompilerParams(vmem_limit_bytes=4 * 2**20),
        name="finish",
    )(*(pltpu.with_memory_space_constraint(a, pltpu.VMEM) for a in arrived))
    return gate.transpose(0, 2, 1), up.transpose(0, 2, 1), sg, su, router.T


def solution(mesh):
    sizes = (2, mesh.shape["ep"] // 2, 2, mesh.shape["fsdp"] // 4, 2)
    split = Mesh(mesh.devices.reshape(sizes), AXES)
    return jax.shard_map(
        functools.partial(per_device, sizes),
        mesh=split,
        in_specs=(
            P(EP, FSDP, None),
            P(EP, FSDP, None),
            P(EP, FSDP, None),
            P(EP, FSDP, None),
            P(FSDP, EP),
            P(FSDP),
        ),
        out_specs=(P(EP, None, FSDP), P(EP, None, FSDP), P(EP, FSDP), P(EP, FSDP), P()),
        check_vma=False,
    )
```

```python
import functools

import jax
import jax.numpy as jnp
from jax import lax
from jax.experimental import pallas as pl
from jax.experimental.pallas import tpu as pltpu
from jax.sharding import Mesh
from jax.sharding import PartitionSpec as P

MESH = pl.DeviceIdType.MESH
AXES = ("zl", "x", "zh", "y", "c")
EP = ("zl", "x")
FSDP = ("zh", "y", "c")
LANES = 128
PEERS = (
    (2, 1, 1), (2, 1, 0), (1, 1, 1), (1, 1, 0), (3, 1, 1), (3, 1, 0), (0, 1, 1), (0, 1, 0),
    (2, 0, 1), (2, 0, 0), (1, 0, 1), (1, 0, 0), (3, 0, 1), (3, 0, 0), (0, 0, 1),
)


def kernel(
    sizes,
    tg, og, tu, ou, rw, rg,
    gate, up, sg, su, router,
    train, other, turned, blocks, first, firsts, local, parts, scales, tiles, weight, gain,
    load_sem, small_sem, send_sem, recv_sem, own_sem,
    first_send, first_recv, part_send, part_recv, scale_send, scale_recv, hand_send,
    tile_send, tile_recv, core_send, core_recv, pair_send, pair_recv, row_send, row_recv,
):
    nzl, nx, nzh, ny, nc = sizes
    experts, depth, width = tg.shape
    members = nzh * ny * nc
    cut = width // members
    strips = width // LANES
    zl, x, zh, y, c = (lax.axis_index(a) for a in AXES)
    me = (zh * ny + y) * nc + c
    arrays = ((tg, og, gate), (tu, ou, up))

    def load(t, e):
        return (
            pltpu.make_async_copy(arrays[t][0].at[e], train.at[t, e], load_sem.at[0, t, e]),
            pltpu.make_async_copy(arrays[t][1].at[e], other.at[t, e], load_sem.at[1, t, e]),
        )

    def peer(step):
        dy, dz, dc = step
        ty, tz, tc = lax.rem(y + dy, ny), lax.rem(zh + dz, nzh), lax.rem(c + dc, nc)
        return (tz * ny + ty) * nc + tc, (zl, x, tz, ty, tc)

    others = [peer(step) for step in PEERS]
    across = (lax.rem(zl + 1, nzl), x, zh, y, c)
    along = [(zl, lax.rem(x + k, nx), zh, y, c) for k in range(1, nx)]
    mine = pl.ds(pl.multiple_of(me * LANES, LANES), LANES)

    barrier = pltpu.get_barrier_semaphore()
    everyone = [d for _, d in others] + [across] + along
    for d in everyone:
        pl.semaphore_signal(barrier, inc=1, device_id=d, device_id_type=MESH)

    for t in range(2):
        for copy in load(t, 0):
            copy.start()
    small = (
        pltpu.make_async_copy(rw, weight, small_sem.at[0]),
        pltpu.make_async_copy(rg, gain, small_sem.at[1]),
    )
    for copy in small:
        copy.start()

    @pl.loop(1, experts)
    def _(e):
        for t in range(2):
            for copy in load(t, e):
                copy.start()

    def largest(t, e):
        for copy in load(t, e):
            copy.wait()
        latest = train[t, e] + other[t, e].astype(jnp.float32)
        return jnp.max(jnp.abs(latest), axis=0, keepdims=True)

    for t in range(2):
        top = largest(t, 0)
        for k in range(strips):
            first[t, k : k + 1, :] = top[:, k * LANES : (k + 1) * LANES]
        firsts[t, me] = first[t]
        if t == 0:
            pl.semaphore_wait(barrier, len(everyone))
        else:
            for copy in small:
                copy.wait()
            tiles[zl] = (weight[...] * gain[...]).astype(tiles.dtype)
        for _, d in others:
            pltpu.make_async_remote_copy(
                first.at[t], firsts.at[t, me], first_send.at[t], first_recv.at[t],
                device_id=d, device_id_type=MESH,
            ).start()
    handed = pltpu.make_async_remote_copy(
        tiles.at[zl], tiles.at[zl], pair_send, pair_recv, device_id=across, device_id_type=MESH
    )
    handed.start()

    def turn(t, e):
        for k in range(strips):
            lanes = slice(k * LANES, (k + 1) * LANES)
            latest = train[t, e, :, lanes] + other[t, e, :, lanes].astype(jnp.float32)
            turned[t, lanes, :] = latest.T

    turn(0, 0)

    @pl.loop(1, experts)
    def _(e):
        for t in range(2):
            chunk = t * experts + e
            top = largest(t, e)
            for k in range(strips):
                local[chunk, k : k + 1, :] = top[:, k * LANES : (k + 1) * LANES]
            owner = chunk
            home = (zl, x, owner // (ny * nc), lax.rem(owner // nc, ny), lax.rem(owner, nc))

            @pl.when(owner != me)
            def _():
                pltpu.make_async_remote_copy(
                    local.at[chunk], parts.at[me], part_send, part_recv,
                    device_id=home, device_id_type=MESH,
                ).start()

            @pl.when(owner == me)
            def _():
                parts[me] = local[chunk]

    def deliver(t, e):
        chunk = t * experts + e
        for p, d in others:
            pltpu.make_async_remote_copy(
                blocks.at[p, chunk], arrays[t][2].at[e, :, mine], send_sem, recv_sem,
                device_id=d, device_id_type=MESH,
            ).start()
        pltpu.make_async_copy(
            blocks.at[me, chunk], arrays[t][2].at[e, :, mine], own_sem.at[0]
        ).start()

    def send(t, e):
        chunk = t * experts + e
        inverse = 1.0 / scales[chunk]
        for k in range(strips):
            lanes = slice(k * LANES, (k + 1) * LANES)
            latest = train[t, e, :, lanes] + other[t, e, :, lanes].astype(jnp.float32)
            turned[t, lanes, :] = (latest * inverse[k : k + 1, :]).T
        for p in range(members):
            blocks[p, chunk] = turned[t, p * cut : (p + 1) * cut, :].astype(blocks.dtype)
        deliver(t, e)

    def send_first(t):
        got = firsts.at[t, pl.ds(0, members - 1)]
        pltpu.make_async_copy(got, got, first_recv.at[t]).wait()
        scale = jnp.max(firsts[t], axis=0)
        scales[t * experts] = scale
        inverse = (1.0 / scale).T
        for p in range(members):
            pieces, row = [], p * cut
            while row < (p + 1) * cut:
                k = row // LANES
                end = min((k + 1) * LANES, (p + 1) * cut)
                column = inverse[row - k * LANES : end - k * LANES, k : k + 1]
                pieces.append(turned[t, row:end, :] * column)
                row = end
            blocks[p, t * experts] = jnp.concatenate(pieces, axis=0).astype(blocks.dtype)
        deliver(t, 0)

    handed.wait()
    bands = [pl.ds(pl.multiple_of((h * nx + x) * 8, 8), 8) for h in range(nzl)]
    for (_, d), step in zip(others, PEERS):
        if step[2] == 0:
            for h, band in enumerate(bands):
                pltpu.make_async_remote_copy(
                    tiles.at[h], router.at[band, mine], tile_send, tile_recv,
                    device_id=d, device_id_type=MESH,
                ).start()
    kept = [
        pltpu.make_async_copy(tiles.at[h], router.at[band, mine], own_sem.at[1 + h])
        for h, band in enumerate(bands)
    ]
    for copy in kept:
        copy.start()
    send_first(0)
    turn(1, 0)

    owns = lax.rem(me, experts) != 0

    @pl.when(owns)
    def _():
        got = parts.at[pl.ds(0, members - 1)]
        pltpu.make_async_copy(got, got, part_recv).wait()
        scales[me] = jnp.max(parts[...], axis=0)
        for (_, d), step in zip(others, PEERS):
            if step[2] == 0 or step == PEERS[-1]:
                pltpu.make_async_remote_copy(
                    scales.at[me], scales.at[me], scale_send, scale_recv.at[me],
                    device_id=d, device_id_type=MESH,
                ).start()

    send_first(1)

    mate = others[-1][1]
    chips = members // nc
    for copy in kept:
        copy.wait()
    row = router.at[pl.ds(0, nzl * 8), pl.ds(0, (chips - 1) * LANES)]
    pltpu.make_async_copy(row, row, tile_recv).wait()
    for q in range(chips):
        lanes = pl.ds(pl.multiple_of((q * nc + c) * LANES, LANES), LANES)
        for band in bands:
            pltpu.make_async_remote_copy(
                router.at[band, lanes], router.at[band, lanes], core_send, core_recv,
                device_id=mate, device_id_type=MESH,
            ).start()
    half = router.at[pl.ds(0, nzl * 8), pl.ds(0, chips * LANES)]

    @pl.loop(1, experts)
    def _(e):
        @pl.when(e == 2)
        def _():
            pltpu.make_async_copy(half, half, core_recv).wait()
            for d in along:
                for band in bands:
                    pltpu.make_async_remote_copy(
                        router.at[band], router.at[band], row_send, row_recv,
                        device_id=d, device_id_type=MESH,
                    ).start()

        for t in range(2):
            chunk = t * experts + e

            @pl.when(chunk != me)
            def _():
                pltpu.make_async_copy(
                    scales.at[chunk], scales.at[chunk], scale_recv.at[chunk]
                ).wait()

                @pl.when(lax.rem(chunk, nc) == c)
                def _():
                    pltpu.make_async_remote_copy(
                        scales.at[chunk], scales.at[chunk], hand_send, scale_recv.at[chunk],
                        device_id=mate, device_id_type=MESH,
                    ).start()

            send(t, e)

    for t, out in enumerate((sg, su)):
        whole = jnp.concatenate(
            [scales[t * experts : (t + 1) * experts, k, :] for k in range(strips)], axis=1
        )
        for p in range(members):

            @pl.when(me == p)
            def _(out=out, whole=whole, p=p):
                out[...] = whole[:, p * cut : (p + 1) * cut]

    def drain(ref, sem):
        pltpu.make_async_copy(ref, ref, sem).wait()

    for t in range(2):
        drain(firsts.at[t, pl.ds(0, members - 1)], first_send.at[t])
    drain(row, tile_send)
    drain(half, core_send)

    @pl.when(owns)
    def _():
        drain(local.at[pl.ds(0, members - 3)], part_send)
        drain(firsts.at[0, pl.ds(0, members // nc)], scale_send)

    @pl.when(jnp.logical_not(owns))
    def _():
        drain(local.at[pl.ds(0, members - 2)], part_send)

    for k in range(nc):
        handed_on = 2 * len([e for e in range(1, experts) if e % nc == k])
        for less in range(2):

            @pl.when(jnp.logical_and(c == k, owns == (less == 1)))
            def _(rows=handed_on - less):
                drain(local.at[pl.ds(0, rows)], hand_send)

    count = nzl * (nx - 1) * 8
    drain(router.at[pl.ds(0, count)], row_send)
    drain(router.at[pl.ds(0, count)], row_recv)
    drain(blocks.at[0], own_sem.at[0])
    drain(blocks.at[pl.ds(0, members - 1)], send_sem)
    drain(blocks.at[pl.ds(0, members - 1)], recv_sem)


def finish(*refs):
    n = len(refs) // 2
    arrived, outs, sem = refs[:n], refs[n:-1], refs[-1]
    copies = []
    for source, out in zip(arrived, outs):
        if len(source.shape) == 3:
            pieces = [(source.at[e], out.at[e]) for e in range(source.shape[0])]
        else:
            pieces = [(source, out)]
        copies += [
            pltpu.make_async_copy(a, b, sem.at[len(copies) + k]) for k, (a, b) in enumerate(pieces)
        ]
    for copy in copies:
        copy.start()
    for copy in copies:
        copy.wait()


def per_device(sizes, train_gate, other_gate, train_up, other_up, router_weight, router_gain):
    experts, depth, width = train_gate.shape
    members = sizes[2] * sizes[3] * sizes[4]
    parts = sizes[0] * sizes[1]
    cut = width // members
    strips = width // LANES
    chunks = 2 * experts
    dma, bf16, f32 = pltpu.SemaphoreType.DMA, jnp.bfloat16, jnp.float32
    hbm = pl.BlockSpec(memory_space=pltpu.HBM)
    vmem = pl.BlockSpec(memory_space=pltpu.VMEM)
    shapes = (
        ((experts, cut, depth * members), bf16),
        ((experts, cut, depth * members), bf16),
        ((experts, cut), f32),
        ((experts, cut), f32),
        ((8 * parts, depth * members), bf16),
    )
    operands = (train_gate, other_gate, train_up, other_up, router_weight.T, router_gain[None])
    arrived = pl.pallas_call(
        functools.partial(kernel, sizes),
        out_shape=[pltpu.VMEM(*shape) for shape in shapes],
        in_specs=[hbm] * 6,
        out_specs=[vmem] * 5,
        scratch_shapes=[
            pltpu.VMEM((2, experts, depth, width), f32),
            pltpu.VMEM((2, experts, depth, width), bf16),
            pltpu.VMEM((2, width, depth), f32),
            pltpu.VMEM((members, chunks, cut, depth), bf16),
            pltpu.VMEM((2, strips, LANES), f32),
            pltpu.VMEM((2, members, strips, LANES), f32),
            pltpu.VMEM((chunks, strips, LANES), f32),
            pltpu.VMEM((members, strips, LANES), f32),
            pltpu.VMEM((chunks, strips, LANES), f32),
            pltpu.VMEM((sizes[0], 8, depth), bf16),
            pltpu.VMEM((8, depth), f32),
            pltpu.VMEM((1, depth), f32),
            dma((2, 2, experts)), dma((2,)),
            dma, dma, dma((1 + sizes[0],)),
            dma((2,)), dma((2,)), dma, dma, dma, dma((chunks,)), dma,
            dma, dma, dma, dma, dma, dma, dma, dma,
        ],
        compiler_params=pltpu.CompilerParams(
            collective_id=0, has_side_effects=True, vmem_limit_bytes=48 * 2**20
        ),
        name="regroup",
    )(*(pltpu.with_memory_space_constraint(a, pltpu.HBM) for a in operands))
    gate, up, sg, su, router = pl.pallas_call(
        finish,
        out_shape=[jax.ShapeDtypeStruct(*shape) for shape in shapes],
        in_specs=[vmem] * 5,
        out_specs=[hbm] * 5,
        scratch_shapes=[dma((2 * experts + 3,))],
        compiler_params=pltpu.CompilerParams(vmem_limit_bytes=4 * 2**20),
        name="finish",
    )(*(pltpu.with_memory_space_constraint(a, pltpu.VMEM) for a in arrived))
    return gate.transpose(0, 2, 1), up.transpose(0, 2, 1), sg, su, router.T


def solution(mesh):
    sizes = (2, mesh.shape["ep"] // 2, 2, mesh.shape["fsdp"] // 4, 2)
    split = Mesh(mesh.devices.reshape(sizes), AXES)
    return jax.shard_map(
        functools.partial(per_device, sizes),
        mesh=split,
        in_specs=(
            P(EP, FSDP, None),
            P(EP, FSDP, None),
            P(EP, FSDP, None),
            P(EP, FSDP, None),
            P(FSDP, EP),
            P(FSDP),
        ),
        out_specs=(P(EP, None, FSDP), P(EP, None, FSDP), P(EP, FSDP), P(EP, FSDP), P()),
        check_vma=False,
    )
```

```python
import functools

import jax
import jax.numpy as jnp
from jax import lax
from jax.experimental import pallas as pl
from jax.experimental.pallas import tpu as pltpu
from jax.sharding import Mesh
from jax.sharding import PartitionSpec as P

MESH = pl.DeviceIdType.MESH
AXES = ("zl", "x", "zh", "y", "c")
EP = ("zl", "x")
FSDP = ("zh", "y", "c")
LANES = 128
PEERS = (
    (2, 1, 1), (2, 1, 0), (1, 1, 1), (1, 1, 0), (3, 1, 1), (3, 1, 0), (0, 1, 1), (0, 1, 0),
    (2, 0, 1), (2, 0, 0), (1, 0, 1), (1, 0, 0), (3, 0, 1), (3, 0, 0), (0, 0, 1),
)


def kernel(
    sizes,
    tg, og, tu, ou, rw, rg,
    gate, up, sg, su, router,
    train, other, turned, blocks, first, firsts, local, parts, scales, tiles, weight, gain, halves,
    load_sem, small_sem, send_sem, recv_sem, own_sem,
    first_send, first_recv, part_send, part_recv, scale_send, scale_recv, hand_send,
    tile_send, tile_recv, core_send, core_recv, swap_send, swap_recv, pair_send, pair_recv, row_send, row_recv,
):
    nzl, nx, nzh, ny, nc = sizes
    experts, depth, width = tg.shape
    members = nzh * ny * nc
    cut = width // members
    strips = width // LANES
    zl, x, zh, y, c = (lax.axis_index(a) for a in AXES)
    chip = zh * ny + y
    chips = members // nc
    me = chip * nc + c
    arrays = ((tg, og, gate), (tu, ou, up))

    def load(t, e):
        return (
            pltpu.make_async_copy(arrays[t][0].at[e], train.at[t, e], load_sem.at[0, t, e]),
            pltpu.make_async_copy(arrays[t][1].at[e], other.at[t, e], load_sem.at[1, t, e]),
        )

    def peer(step):
        dy, dz, dc = step
        ty, tz, tc = lax.rem(y + dy, ny), lax.rem(zh + dz, nzh), lax.rem(c + dc, nc)
        return (tz * ny + ty) * nc + tc, (zl, x, tz, ty, tc)

    others = [peer(step) for step in PEERS]
    across = (lax.rem(zl + 1, nzl), x, zh, y, c)
    along = [(zl, lax.rem(x + k, nx), zh, y, c) for k in range(1, nx)]
    mate = others[-1][1]
    mine = pl.ds(pl.multiple_of(me * LANES, LANES), LANES)

    barrier = pltpu.get_barrier_semaphore()
    everyone = [d for _, d in others] + [across] + along
    for d in everyone:
        pl.semaphore_signal(barrier, inc=1, device_id=d, device_id_type=MESH)

    for t in range(2):
        for copy in load(t, 0):
            copy.start()
    small = (
        pltpu.make_async_copy(rw, weight, small_sem.at[0]),
        pltpu.make_async_copy(rg, gain, small_sem.at[1]),
    )
    for copy in small:
        copy.start()

    @pl.loop(1, experts)
    def _(e):
        for t in range(2):
            for copy in load(t, e):
                copy.start()

    def largest(t, e):
        for copy in load(t, e):
            copy.wait()
        latest = train[t, e] + other[t, e].astype(jnp.float32)
        return jnp.max(jnp.abs(latest), axis=0, keepdims=True)

    for t in range(2):
        top = largest(t, 0)
        for k in range(strips):
            first[t, k : k + 1, :] = top[:, k * LANES : (k + 1) * LANES]
        firsts[t, (me, chip)[t]] = first[t]
        if t == 0:
            pl.semaphore_wait(barrier, len(everyone))
        else:
            for copy in small:
                copy.wait()
            tiles[zl] = (weight[...] * gain[...]).astype(tiles.dtype)
        for (_, d), step in zip(others, PEERS):
            if t == 0 or step[2] == 0:
                pltpu.make_async_remote_copy(
                    first.at[t], firsts.at[t, (me, chip)[t]], first_send.at[t], first_recv.at[t],
                    device_id=d, device_id_type=MESH,
                ).start()
    handed = pltpu.make_async_remote_copy(
        tiles.at[zl], tiles.at[zl], pair_send, pair_recv, device_id=across, device_id_type=MESH
    )
    handed.start()

    def turn(t, e):
        for k in range(strips):
            lanes = slice(k * LANES, (k + 1) * LANES)
            latest = train[t, e, :, lanes] + other[t, e, :, lanes].astype(jnp.float32)
            turned[t, lanes, :] = latest.T

    turn(0, 0)

    @pl.loop(1, experts)
    def _(e):
        for t in range(2):
            chunk = t * experts + e
            top = largest(t, e)
            for k in range(strips):
                local[chunk, k : k + 1, :] = top[:, k * LANES : (k + 1) * LANES]
            owner = chunk
            home = (zl, x, owner // (ny * nc), lax.rem(owner // nc, ny), lax.rem(owner, nc))

            @pl.when(owner != me)
            def _():
                pltpu.make_async_remote_copy(
                    local.at[chunk], parts.at[me], part_send, part_recv,
                    device_id=home, device_id_type=MESH,
                ).start()

            @pl.when(owner == me)
            def _():
                parts[me] = local[chunk]

    def deliver(t, e):
        chunk = t * experts + e
        for p, d in others:
            pltpu.make_async_remote_copy(
                blocks.at[p, chunk], arrays[t][2].at[e, :, mine], send_sem, recv_sem,
                device_id=d, device_id_type=MESH,
            ).start()
        pltpu.make_async_copy(
            blocks.at[me, chunk], arrays[t][2].at[e, :, mine], own_sem.at[0]
        ).start()

    def send(t, e):
        chunk = t * experts + e
        inverse = 1.0 / scales[chunk]
        for k in range(strips):
            lanes = slice(k * LANES, (k + 1) * LANES)
            latest = train[t, e, :, lanes] + other[t, e, :, lanes].astype(jnp.float32)
            turned[t, lanes, :] = (latest * inverse[k : k + 1, :]).T
        for p in range(members):
            blocks[p, chunk] = turned[t, p * cut : (p + 1) * cut, :].astype(blocks.dtype)
        deliver(t, e)

    def send_first(t):
        if t == 0:
            got = firsts.at[t, pl.ds(0, members - 1)]
            pltpu.make_async_copy(got, got, first_recv.at[t]).wait()
            scale = jnp.max(firsts[t], axis=0)
        else:
            swapped.wait()
            scale = jnp.maximum(halves[0], halves[1])
        scales[t * experts] = scale
        inverse = (1.0 / scale).T
        for p in range(members):
            pieces, row = [], p * cut
            while row < (p + 1) * cut:
                k = row // LANES
                end = min((k + 1) * LANES, (p + 1) * cut)
                column = inverse[row - k * LANES : end - k * LANES, k : k + 1]
                pieces.append(turned[t, row:end, :] * column)
                row = end
            blocks[p, t * experts] = jnp.concatenate(pieces, axis=0).astype(blocks.dtype)
        deliver(t, 0)

    handed.wait()
    bands = [pl.ds(pl.multiple_of((h * nx + x) * 8, 8), 8) for h in range(nzl)]
    for (_, d), step in zip(others, PEERS):
        if step[2] == 0:
            for h, band in enumerate(bands):
                pltpu.make_async_remote_copy(
                    tiles.at[h], router.at[band, mine], tile_send, tile_recv,
                    device_id=d, device_id_type=MESH,
                ).start()
    kept = [
        pltpu.make_async_copy(tiles.at[h], router.at[band, mine], own_sem.at[1 + h])
        for h, band in enumerate(bands)
    ]
    for copy in kept:
        copy.start()
    send_first(0)

    got = firsts.at[1, pl.ds(0, chips - 1)]
    pltpu.make_async_copy(got, got, first_recv.at[1]).wait()
    halves[0] = jnp.max(firsts[1, 0:chips], axis=0)
    swapped = pltpu.make_async_remote_copy(
        halves.at[0], halves.at[1], swap_send, swap_recv, device_id=mate, device_id_type=MESH
    )
    swapped.start()
    turn(1, 0)

    owns = lax.rem(me, experts) != 0

    @pl.when(owns)
    def _():
        got = parts.at[pl.ds(0, members - 1)]
        pltpu.make_async_copy(got, got, part_recv).wait()
        scales[me] = jnp.max(parts[...], axis=0)
        for (_, d), step in zip(others, PEERS):
            if step[2] == 0 or step == PEERS[-1]:
                pltpu.make_async_remote_copy(
                    scales.at[me], scales.at[me], scale_send, scale_recv.at[me],
                    device_id=d, device_id_type=MESH,
                ).start()

    send_first(1)

    for copy in kept:
        copy.wait()
    row = router.at[pl.ds(0, nzl * 8), pl.ds(0, (chips - 1) * LANES)]
    pltpu.make_async_copy(row, row, tile_recv).wait()
    for q in range(chips):
        lanes = pl.ds(pl.multiple_of((q * nc + c) * LANES, LANES), LANES)
        for band in bands:
            pltpu.make_async_remote_copy(
                router.at[band, lanes], router.at[band, lanes], core_send, core_recv,
                device_id=mate, device_id_type=MESH,
            ).start()
    half = router.at[pl.ds(0, nzl * 8), pl.ds(0, chips * LANES)]

    @pl.loop(1, experts)
    def _(e):
        @pl.when(e == 2)
        def _():
            pltpu.make_async_copy(half, half, core_recv).wait()
            for d in along:
                for band in bands:
                    pltpu.make_async_remote_copy(
                        router.at[band], router.at[band], row_send, row_recv,
                        device_id=d, device_id_type=MESH,
                    ).start()

        for t in range(2):
            chunk = t * experts + e

            @pl.when(chunk != me)
            def _():
                pltpu.make_async_copy(
                    scales.at[chunk], scales.at[chunk], scale_recv.at[chunk]
                ).wait()

                @pl.when(lax.rem(chunk, nc) == c)
                def _():
                    pltpu.make_async_remote_copy(
                        scales.at[chunk], scales.at[chunk], hand_send, scale_recv.at[chunk],
                        device_id=mate, device_id_type=MESH,
                    ).start()

            send(t, e)

    for t, out in enumerate((sg, su)):
        whole = jnp.concatenate(
            [scales[t * experts : (t + 1) * experts, k, :] for k in range(strips)], axis=1
        )
        for p in range(members):

            @pl.when(me == p)
            def _(out=out, whole=whole, p=p):
                out[...] = whole[:, p * cut : (p + 1) * cut]

    def drain(ref, sem):
        pltpu.make_async_copy(ref, ref, sem).wait()

    for t in range(2):
        drain(firsts.at[t, pl.ds(0, (members, chips)[t] - 1)], first_send.at[t])
    drain(row, tile_send)
    drain(half, core_send)

    @pl.when(owns)
    def _():
        drain(local.at[pl.ds(0, members - 3)], part_send)
        drain(firsts.at[0, pl.ds(0, members // nc)], scale_send)

    @pl.when(jnp.logical_not(owns))
    def _():
        drain(local.at[pl.ds(0, members - 2)], part_send)

    for k in range(nc):
        handed_on = 2 * len([e for e in range(1, experts) if e % nc == k])
        for less in range(2):

            @pl.when(jnp.logical_and(c == k, owns == (less == 1)))
            def _(rows=handed_on - less):
                drain(local.at[pl.ds(0, rows)], hand_send)

    count = nzl * (nx - 1) * 8
    drain(router.at[pl.ds(0, count)], row_send)
    drain(router.at[pl.ds(0, count)], row_recv)
    drain(blocks.at[0], own_sem.at[0])
    drain(blocks.at[pl.ds(0, members - 1)], send_sem)
    drain(blocks.at[pl.ds(0, members - 1)], recv_sem)


def finish(*refs):
    n = len(refs) // 2
    arrived, outs, sem = refs[:n], refs[n:-1], refs[-1]
    copies = []
    for source, out in zip(arrived, outs):
        if len(source.shape) == 3:
            pieces = [(source.at[e], out.at[e]) for e in range(source.shape[0])]
        else:
            pieces = [(source, out)]
        copies += [
            pltpu.make_async_copy(a, b, sem.at[len(copies) + k]) for k, (a, b) in enumerate(pieces)
        ]
    for copy in copies:
        copy.start()
    for copy in copies:
        copy.wait()


def per_device(sizes, train_gate, other_gate, train_up, other_up, router_weight, router_gain):
    experts, depth, width = train_gate.shape
    members = sizes[2] * sizes[3] * sizes[4]
    parts = sizes[0] * sizes[1]
    cut = width // members
    strips = width // LANES
    chunks = 2 * experts
    dma, bf16, f32 = pltpu.SemaphoreType.DMA, jnp.bfloat16, jnp.float32
    hbm = pl.BlockSpec(memory_space=pltpu.HBM)
    vmem = pl.BlockSpec(memory_space=pltpu.VMEM)
    shapes = (
        ((experts, cut, depth * members), bf16),
        ((experts, cut, depth * members), bf16),
        ((experts, cut), f32),
        ((experts, cut), f32),
        ((8 * parts, depth * members), bf16),
    )
    operands = (train_gate, other_gate, train_up, other_up, router_weight.T, router_gain[None])
    arrived = pl.pallas_call(
        functools.partial(kernel, sizes),
        out_shape=[pltpu.VMEM(*shape) for shape in shapes],
        in_specs=[hbm] * 6,
        out_specs=[vmem] * 5,
        scratch_shapes=[
            pltpu.VMEM((2, experts, depth, width), f32),
            pltpu.VMEM((2, experts, depth, width), bf16),
            pltpu.VMEM((2, width, depth), f32),
            pltpu.VMEM((members, chunks, cut, depth), bf16),
            pltpu.VMEM((2, strips, LANES), f32),
            pltpu.VMEM((2, members, strips, LANES), f32),
            pltpu.VMEM((chunks, strips, LANES), f32),
            pltpu.VMEM((members, strips, LANES), f32),
            pltpu.VMEM((chunks, strips, LANES), f32),
            pltpu.VMEM((sizes[0], 8, depth), bf16),
            pltpu.VMEM((8, depth), f32),
            pltpu.VMEM((1, depth), f32),
            pltpu.VMEM((2, strips, LANES), f32),
            dma((2, 2, experts)), dma((2,)),
            dma, dma, dma((1 + sizes[0],)),
            dma((2,)), dma((2,)), dma, dma, dma, dma((chunks,)), dma,
            dma, dma, dma, dma, dma, dma, dma, dma, dma, dma,
        ],
        compiler_params=pltpu.CompilerParams(
            collective_id=0, has_side_effects=True, vmem_limit_bytes=48 * 2**20
        ),
        name="regroup",
    )(*(pltpu.with_memory_space_constraint(a, pltpu.HBM) for a in operands))
    gate, up, sg, su, router = pl.pallas_call(
        finish,
        out_shape=[jax.ShapeDtypeStruct(*shape) for shape in shapes],
        in_specs=[vmem] * 5,
        out_specs=[hbm] * 5,
        scratch_shapes=[dma((2 * experts + 3,))],
        compiler_params=pltpu.CompilerParams(vmem_limit_bytes=4 * 2**20),
        name="finish",
    )(*(pltpu.with_memory_space_constraint(a, pltpu.VMEM) for a in arrived))
    return gate.transpose(0, 2, 1), up.transpose(0, 2, 1), sg, su, router.T


def solution(mesh):
    sizes = (2, mesh.shape["ep"] // 2, 2, mesh.shape["fsdp"] // 4, 2)
    split = Mesh(mesh.devices.reshape(sizes), AXES)
    return jax.shard_map(
        functools.partial(per_device, sizes),
        mesh=split,
        in_specs=(
            P(EP, FSDP, None),
            P(EP, FSDP, None),
            P(EP, FSDP, None),
            P(EP, FSDP, None),
            P(FSDP, EP),
            P(FSDP),
        ),
        out_specs=(P(EP, None, FSDP), P(EP, None, FSDP), P(EP, FSDP), P(EP, FSDP), P()),
        check_vma=False,
    )
```
